32 devices in a mesh: row: 8 (over z, x), col: 4 (over y, core).
Axes of the slice: x: 2, y: 2, z: 4, core: 2. Of those that a mesh axis runs over, the one named last changes fastest.
Arguments:
- offsets: int32 [8, 4, 2], P('row', 'col'), may hold values from 1 to 3
- targets: float32 [3, 3, 256, 512], P(None, None, 'row', 'col'), may hold values from -60 to 60
- grid_fine: float32 [32, 256, 512], P(None, 'row', 'col'), may hold values from -6 to 6
- grid_coarse: float32 [32, 64, 128], P(None, 'row', 'col'), may hold values from -6 to 6
- weight_in: float32 [512, 64], replicated, may hold values from -0.75 to 0.75
- weight_mid: float32 [1, 512, 512], replicated, may hold values from -0.25 to 0.25
- weight_out: float32 [3, 512], replicated, may hold values from -0.397747564 to 0.397747564
- fine_first: float32 [32, 256, 512], P(None, 'row', 'col'), may hold values from -0.012 to 0.012
- fine_second: float32 [32, 256, 512], P(None, 'row', 'col'), may hold values from 1e-06 to 0.0001
- coarse_first: float32 [32, 64, 128], P(None, 'row', 'col'), may hold values from -0.012 to 0.012
- coarse_second: float32 [32, 64, 128], P(None, 'row', 'col'), may hold values from 1e-06 to 0.0001
- in_first: float32 [512, 64], replicated, may hold values from -0.012 to 0.012
- in_second: float32 [512, 64], replicated, may hold values from 1e-06 to 0.0001
- mid_first: float32 [1, 512, 512], replicated, may hold values from -0.012 to 0.012
- mid_second: float32 [1, 512, 512], replicated, may hold values from 1e-06 to 0.0001
- out_first: float32 [3, 512], replicated, may hold values from -0.012 to 0.012
- out_second: float32 [3, 512], replicated, may hold values from 1e-06 to 0.0001
Outputs:
- fine_step: float32 [32, 256, 512], P(None, 'row', 'col')
- coarse_step: float32 [32, 64, 128], P(None, 'row', 'col')
- input_step: float32 [512, 64], replicated
- middle_step: float32 [1, 512, 512], replicated
- output_step: float32 [3, 512], replicated
The draws below stay inside these ranges and needn't reach their ends.
All inputs are finite; a program needn't handle non-finite values.
Results may differ from the reference program's by a relative error of at most 0.0014.
The reference program's roundings to bfloat16 on the way count: a program that leaves them out, or rounds other values in their place, can miss the bound.
Values sent between devices are 32-bit elements; how exact they have to be, the bound alone decides.
A program may use at most 64 MiB of HBM per device.

```python
import math
import jax
import jax.numpy as jnp
from jax import lax

CH = 32
HID = 512
MID = 1
OUT = 3
SUB = 4
RATIO = 4
ADAM_STEP = 10
SR = 32
SC = 128
TILE_ROWS = 8
TILE_COLS = 4
ROWS = 256
COLS = 512
CROWS = 64
CCOLS = 128
N_ROW = 8
N_COL = 4


def draw_targets(key, part):
    row_level = jnp.arange(ROWS, dtype=jnp.float32) / ROWS
    col_level = jnp.arange(COLS, dtype=jnp.float32) / COLS
    exponent = 0.5 * (row_level[:, None] + col_level[None, :])
    noise = jnp.clip(jax.random.normal(key, (3, OUT, ROWS, COLS), jnp.float32), -4.0, 4.0)
    return noise * 10.0 ** exponent


def draw_weight_out(key, part):
    column_level = 0.3 * 10.0 ** (jnp.arange(HID, dtype=jnp.float32) / (HID - 1))
    noise = jnp.clip(jax.random.normal(key, (OUT, HID), jnp.float32), -3.0, 3.0)
    return noise * column_level[None, :] / HID ** 0.5


def set_ends(values, key, least, top_value):
    extent = values.shape
    index_at = [jax.random.randint(jax.random.fold_in(key, axis), (), 0, extent[axis]) for axis in range(len(extent))]
    values = values.at[tuple(index_at)].set(least)
    longest = extent.index(max(extent))
    index_at[longest] = (index_at[longest] + 1) % extent[longest]
    return values.at[tuple(index_at)].set(top_value)


def block_levels(key, extent, pieces, smallest, top_value):
    level = 1.0
    for axis_at, parts in pieces:
        steps = jax.random.uniform(jax.random.fold_in(jax.random.fold_in(key, 6), axis_at), (parts,), jnp.float32, smallest / len(pieces), top_value / len(pieces))
        level = level * jnp.repeat(jnp.exp(steps), extent[axis_at] // parts).reshape((-1,) + (1,) * (len(extent) - 1 - axis_at))
    return level


def scatter_about(own_key, dims, deviation, reach, split=(), held_as=jnp.bfloat16):
    result = deviation * jax.random.normal(own_key, dims, jnp.float32)
    if split:
        result = result * block_levels(own_key, dims, split, -0.22, 0.18)
    return jnp.clip(result, -reach, reach).astype(held_as)


def setup_inputs(seed: int = 0) -> dict:
    key_of = jax.random.split(jax.random.key(seed), 18)
    return {
        "offsets": set_ends(jax.random.randint(key_of[0], (TILE_ROWS, TILE_COLS, 2), 1, SUB), jax.random.fold_in(key_of[0], 1), 1, SUB - 1).astype(jnp.int32),
        "targets": draw_targets(jax.random.fold_in(key_of[17], 71), 0),
        "grid_fine": scatter_about(key_of[2], (CH, ROWS, COLS), 1.0, 6.0, ((1, 8), (2, 4)), jnp.float32),
        "grid_coarse": scatter_about(key_of[3], (CH, CROWS, CCOLS), 1.0, 6.0, ((1, 8), (2, 4)), jnp.float32),
        "weight_in": scatter_about(key_of[4], (HID, 2 * CH), (2 * CH) ** -0.5, 0.75, (), jnp.float32),
        "weight_mid": scatter_about(key_of[5], (MID, HID, HID), HID ** -0.5, 0.25, (), jnp.float32),
        "weight_out": draw_weight_out(jax.random.fold_in(key_of[17], 71), 0),
        "fine_first": scatter_about(key_of[7], (CH, ROWS, COLS), 0.002, 0.012, ((1, 8), (2, 4)), jnp.float32),
        "fine_second": jnp.clip(jnp.exp(math.log(0.0001) - 4.6051702 * jax.random.uniform(key_of[8], (CH, ROWS, COLS), jnp.float32) ** block_levels(key_of[8], (CH, ROWS, COLS), ((1, 8), (2, 4)), -0.2, 0.2)), 9.999999974752427e-07, 0.0001),
        "coarse_first": scatter_about(key_of[9], (CH, CROWS, CCOLS), 0.002, 0.012, ((1, 8), (2, 4)), jnp.float32),
        "coarse_second": jnp.clip(jnp.exp(math.log(0.0001) - 4.6051702 * jax.random.uniform(key_of[10], (CH, CROWS, CCOLS), jnp.float32) ** block_levels(key_of[10], (CH, CROWS, CCOLS), ((1, 8), (2, 4)), -0.2, 0.2)), 9.999999974752427e-07, 0.0001),
        "in_first": scatter_about(key_of[11], (HID, 2 * CH), 0.002, 0.012, (), jnp.float32),
        "in_second": jnp.clip(jnp.exp(jax.random.uniform(key_of[12], (HID, 2 * CH), jnp.float32, math.log(9.999999974752427e-07), math.log(0.0001))), 9.999999974752427e-07, 0.0001),
        "mid_first": scatter_about(key_of[13], (MID, HID, HID), 0.002, 0.012, (), jnp.float32),
        "mid_second": jnp.clip(jnp.exp(jax.random.uniform(key_of[14], (MID, HID, HID), jnp.float32, math.log(9.999999974752427e-07), math.log(0.0001))), 9.999999974752427e-07, 0.0001),
        "out_first": scatter_about(key_of[15], (OUT, HID), 0.002, 0.012, (), jnp.float32),
        "out_second": jnp.clip(jnp.exp(jax.random.uniform(key_of[16], (OUT, HID), jnp.float32, math.log(9.999999974752427e-07), math.log(0.0001))), 9.999999974752427e-07, 0.0001),
    }


BETA_ONE = 0.9
BETA_TWO = 0.99
ADAM_EPSILON = 1e-08
CLIP_RMS = 0.01
LOSS_VALUE = 0.25
MEAN_EPSILON = 1e-06

def interp_table(samples, level_ratio, offset):
    positions = jnp.arange(samples, dtype=jnp.int32)
    base_index = positions // level_ratio
    fraction = ((positions % level_ratio).astype(jnp.float32) + offset.astype(jnp.float32) / SUB) / level_ratio
    column = jnp.arange(samples // level_ratio + 1, dtype=jnp.int32)
    lower_hit = (column[None, :] == base_index[:, None]).astype(jnp.float32)
    upper_hit = (column[None, :] == base_index[:, None] + 1).astype(jnp.float32)
    return lower_hit * (1.0 - fraction)[:, None] + upper_hit * fraction[:, None]

def level_tables(row_count, col_count, shift_y, shift_x):
    return (interp_table(row_count, 1, shift_y), interp_table(col_count, 1, shift_x), interp_table(row_count, RATIO, shift_y), interp_table(col_count, RATIO, shift_x))

def sample_level(extended, row_table, col_table):
    across = jnp.einsum('kjl,ml->kjm', extended, col_table, precision=lax.Precision.HIGHEST)
    return jnp.einsum('ij,kjm->kim', row_table, across, precision=lax.Precision.HIGHEST)

def spread_level(cotangent, row_table, col_table):
    backward = jnp.einsum('ij,kim->kjm', row_table, cotangent, precision=lax.Precision.HIGHEST)
    return jnp.einsum('kjm,ml->kjl', backward, col_table, precision=lax.Precision.HIGHEST)

def sample_features(fine_ext, coarse_ext, tables):
    fine_feat = sample_level(fine_ext, tables[0], tables[1])
    coarse_feat = sample_level(coarse_ext, tables[2], tables[3])
    channels, row_count, col_count = fine_feat.shape
    return jnp.concatenate([fine_feat.reshape(channels, row_count * col_count), coarse_feat.reshape(channels, row_count * col_count)], axis=0).astype(jnp.bfloat16)

def spread_features(feature_grad, tables):
    channels = feature_grad.shape[0] // 2
    row_count = tables[0].shape[0]
    col_count = tables[1].shape[0]
    fine_cot = feature_grad[:channels].reshape(channels, row_count, col_count)
    coarse_cot = feature_grad[channels:].reshape(channels, row_count, col_count)
    return (spread_level(fine_cot, tables[0], tables[1]), spread_level(coarse_cot, tables[2], tables[3]))

def matmul(former, latter):
    return jnp.dot(former, latter, preferred_element_type=jnp.float32)

def contract_rows(former, latter):
    return lax.dot_general(former, latter, (((0,), (0,)), ((), ())), preferred_element_type=jnp.float32)

def contract_cols(former, latter):
    return lax.dot_general(former, latter, (((1,), (1,)), ((), ())), preferred_element_type=jnp.float32)

def silu_slope(pre_act):
    sigmoid = jax.nn.sigmoid(pre_act)
    return sigmoid * (1.0 + pre_act * (1.0 - sigmoid))

def decoder_forward(features, low_in, low_mid, low_out):
    pre_acts = [matmul(low_in, features)]
    activations = [jax.nn.silu(pre_acts[0]).astype(jnp.bfloat16)]
    for layer_index in range(low_mid.shape[0]):
        pre_acts.append(matmul(low_mid[layer_index], activations[-1]))
        activations.append(jax.nn.silu(pre_acts[-1]).astype(jnp.bfloat16))
    return (matmul(low_out, activations[-1]), pre_acts, activations)

def decoder_backward(features, pre_acts, activations, cotangent, low_in, low_mid, low_out):
    out_cotangent = cotangent.astype(jnp.bfloat16)
    grad_out = contract_cols(out_cotangent, activations[-1])
    upward = contract_rows(low_out, out_cotangent)
    grads_mid = []
    for layer_index in range(low_mid.shape[0] - 1, -1, -1):
        delta_low = (upward * silu_slope(pre_acts[layer_index + 1])).astype(jnp.bfloat16)
        grads_mid.insert(0, contract_cols(delta_low, activations[layer_index]))
        upward = contract_rows(low_mid[layer_index], delta_low)
    delta_low = (upward * silu_slope(pre_acts[0])).astype(jnp.bfloat16)
    grad_in = contract_cols(delta_low, features)
    feature_grad = contract_rows(low_in, delta_low)
    return (grad_in, jnp.stack(grads_mid), grad_out, feature_grad)

def pixel_cotangent(value_error, row_error, row_prior, col_error, col_prior):
    return 2.0 * LOSS_VALUE * value_error + 2.0 * (row_prior - row_error) + 2.0 * (col_prior - col_error)

def clip_factor(total, entries):
    return jnp.minimum(1.0, CLIP_RMS / jnp.sqrt(total / entries + MEAN_EPSILON))

def adam_step(gradient, moment_one, moment_two, clip_scale):
    clipped = gradient * clip_scale
    new_one = BETA_ONE * moment_one + (1.0 - BETA_ONE) * clipped
    new_two = BETA_TWO * moment_two + (1.0 - BETA_TWO) * clipped * clipped
    return new_one / (1.0 - BETA_ONE ** ADAM_STEP) / (jnp.sqrt(new_two / (1.0 - BETA_TWO ** ADAM_STEP)) + ADAM_EPSILON)

def reference(offsets, targets, grid_fine, grid_coarse, weight_in, weight_mid, weight_out, fine_first, fine_second, coarse_first, coarse_second, in_first, in_second, mid_first, mid_second, out_first, out_second):
    tile_count = N_ROW * N_COL
    coarse_tile_rows = SR // RATIO
    coarse_tile_cols = SC // RATIO
    fine_padded = jnp.pad(grid_fine, ((0, 0), (0, 1), (0, 1)))
    coarse_padded = jnp.pad(grid_coarse, ((0, 0), (0, 1), (0, 1)))
    low_in = weight_in.astype(jnp.bfloat16)
    low_mid = weight_mid.astype(jnp.bfloat16)
    low_out = weight_out.astype(jnp.bfloat16)
    zero_index = jnp.zeros((), jnp.int32)

    def tile_starts(tile_index):
        row_tile = (tile_index // N_COL).astype(jnp.int32)
        col_tile = (tile_index % N_COL).astype(jnp.int32)
        return (row_tile, col_tile)

    def tile_forward(tile_index):
        row_tile, col_tile = tile_starts(tile_index)
        fine_ext = lax.dynamic_slice(fine_padded, (zero_index, row_tile * SR, col_tile * SC), (CH, SR + 1, SC + 1))
        coarse_ext = lax.dynamic_slice(coarse_padded, (zero_index, row_tile * coarse_tile_rows, col_tile * coarse_tile_cols), (CH, coarse_tile_rows + 1, coarse_tile_cols + 1))
        tables = level_tables(SR, SC, offsets[row_tile, col_tile, 0], offsets[row_tile, col_tile, 1])
        features = sample_features(fine_ext, coarse_ext, tables)
        predicted, pre_acts, activations = decoder_forward(features, low_in, low_mid, low_out)
        return (predicted, features, pre_acts, activations, tables)
    tile_range = jnp.arange(tile_count, dtype=jnp.int32)
    tile_preds = lax.map(lambda tile_index: tile_forward(tile_index)[0], tile_range)
    predicted = tile_preds.reshape(N_ROW, N_COL, OUT, SR, SC).transpose(2, 0, 3, 1, 4).reshape(OUT, ROWS, COLS)
    value_error = predicted - targets[0]
    row_error = jnp.pad(predicted[:, 1:, :] - predicted[:, :-1, :] - targets[1][:, :-1, :], ((0, 0), (0, 1), (0, 0)))
    col_error = jnp.pad(predicted[:, :, 1:] - predicted[:, :, :-1] - targets[2][:, :, :-1], ((0, 0), (0, 0), (0, 1)))
    row_prior = jnp.pad(row_error[:, :-1, :], ((0, 0), (1, 0), (0, 0)))
    col_prior = jnp.pad(col_error[:, :, :-1], ((0, 0), (0, 0), (1, 0)))
    cotangent = pixel_cotangent(value_error, row_error, row_prior, col_error, col_prior)
    tile_cots = cotangent.reshape(OUT, N_ROW, SR, N_COL, SC).transpose(1, 3, 0, 2, 4).reshape(tile_count, OUT, SR * SC)

    def tile_backward(running, inputs):
        tile_index, tile_cot = inputs
        unused_pred, features, pre_acts, activations, tables = tile_forward(tile_index)
        grad_in, grad_mid, grad_out, feature_grad = decoder_backward(features, pre_acts, activations, tile_cot, low_in, low_mid, low_out)
        fine_back, coarse_back = spread_features(feature_grad, tables)
        sum_in, sum_mid, sum_out, fine_acc, coarse_acc = running
        row_tile, col_tile = tile_starts(tile_index)
        fine_start = (zero_index, row_tile * SR, col_tile * SC)
        coarse_start = (zero_index, row_tile * coarse_tile_rows, col_tile * coarse_tile_cols)
        fine_acc = lax.dynamic_update_slice(fine_acc, lax.dynamic_slice(fine_acc, fine_start, fine_back.shape) + fine_back, fine_start)
        coarse_acc = lax.dynamic_update_slice(coarse_acc, lax.dynamic_slice(coarse_acc, coarse_start, coarse_back.shape) + coarse_back, coarse_start)
        return ((sum_in + grad_in, sum_mid + grad_mid, sum_out + grad_out, fine_acc, coarse_acc), None)
    initial = (jnp.zeros(weight_in.shape, jnp.float32), jnp.zeros(weight_mid.shape, jnp.float32), jnp.zeros(weight_out.shape, jnp.float32), jnp.zeros((CH, ROWS + 1, COLS + 1), jnp.float32), jnp.zeros((CH, CROWS + 1, CCOLS + 1), jnp.float32))
    finals, unused_stack = lax.scan(tile_backward, initial, (tile_range, tile_cots))
    grad_in, grad_mid, grad_out, fine_acc, coarse_acc = finals
    fine_grad = fine_acc[:, :ROWS, :COLS]
    coarse_grad = coarse_acc[:, :CROWS, :CCOLS]
    grid_total = jnp.sum(fine_grad * fine_grad) + jnp.sum(coarse_grad * coarse_grad)
    grid_scale = clip_factor(grid_total, CH * (ROWS * COLS + CROWS * CCOLS))
    decoder_total = jnp.sum(grad_in * grad_in) + jnp.sum(grad_mid * grad_mid) + jnp.sum(grad_out * grad_out)
    decoder_scale = clip_factor(decoder_total, weight_in.size + weight_mid.size + weight_out.size)
    fine_step = adam_step(fine_grad, fine_first, fine_second, grid_scale)
    coarse_step = adam_step(coarse_grad, coarse_first, coarse_second, grid_scale)
    input_step = adam_step(grad_in, in_first, in_second, decoder_scale)
    middle_step = adam_step(grad_mid, mid_first, mid_second, decoder_scale)
    output_step = adam_step(grad_out, out_first, out_second, decoder_scale)
    return (fine_step, coarse_step, input_step, middle_step, output_step)
```

```python
import jax
import jax.numpy as jnp
from jax import lax
from jax.experimental import pallas as pl
from jax.experimental.pallas import tpu as pltpu
from jax.sharding import PartitionSpec as P

SUB = 4
RATIO = 4
ADAM_STEP = 10


BETA_ONE = 0.9
BETA_TWO = 0.99
ADAM_EPSILON = 1e-08
CLIP_RMS = 0.01
LOSS_VALUE = 0.25
MEAN_EPSILON = 1e-06


def shifted(block, axis, distance):
    devices = range(lax.axis_size(axis))
    route = [(i - distance, i) for i in devices if i - distance in devices]
    return lax.ppermute(block, axis, route)


def interp_table(samples, level_ratio, offset):
    positions = jnp.arange(samples, dtype=jnp.int32)
    base_index = positions // level_ratio
    fraction = (
        (positions % level_ratio).astype(jnp.float32) + offset.astype(jnp.float32) / SUB
    ) / level_ratio
    column = jnp.arange(samples // level_ratio + 1, dtype=jnp.int32)
    lower_hit = (column[None, :] == base_index[:, None]).astype(jnp.float32)
    upper_hit = (column[None, :] == base_index[:, None] + 1).astype(jnp.float32)
    return lower_hit * (1.0 - fraction)[:, None] + upper_hit * fraction[:, None]


def level_tables(row_count, col_count, shift_y, shift_x):
    return (
        interp_table(row_count, 1, shift_y),
        interp_table(col_count, 1, shift_x),
        interp_table(row_count, RATIO, shift_y),
        interp_table(col_count, RATIO, shift_x),
    )


def sample_level(extended, row_table, col_table):
    across = jnp.einsum("kjl,ml->kjm", extended, col_table, precision=lax.Precision.HIGHEST)
    return jnp.einsum("ij,kjm->kim", row_table, across, precision=lax.Precision.HIGHEST)


def spread_level(cotangent, row_table, col_table):
    backward = jnp.einsum("ij,kim->kjm", row_table, cotangent, precision=lax.Precision.HIGHEST)
    return jnp.einsum("kjm,ml->kjl", backward, col_table, precision=lax.Precision.HIGHEST)


def sample_features(fine_ext, coarse_ext, tables):
    fine_feat = sample_level(fine_ext, tables[0], tables[1])
    coarse_feat = sample_level(coarse_ext, tables[2], tables[3])
    channels, row_count, col_count = fine_feat.shape
    return jnp.concatenate(
        [
            fine_feat.reshape(channels, row_count * col_count),
            coarse_feat.reshape(channels, row_count * col_count),
        ],
        axis=0,
    ).astype(jnp.bfloat16)


def spread_features(feature_grad, tables):
    channels = feature_grad.shape[0] // 2
    row_count = tables[0].shape[0]
    col_count = tables[1].shape[0]
    fine_cot = feature_grad[:channels].reshape(channels, row_count, col_count)
    coarse_cot = feature_grad[channels:].reshape(channels, row_count, col_count)
    return (
        spread_level(fine_cot, tables[0], tables[1]),
        spread_level(coarse_cot, tables[2], tables[3]),
    )


def matmul(former, latter):
    return jnp.dot(former, latter, preferred_element_type=jnp.float32)


def contract_rows(former, latter):
    return lax.dot_general(
        former, latter, (((0,), (0,)), ((), ())), preferred_element_type=jnp.float32
    )


def contract_cols(former, latter):
    return lax.dot_general(
        former, latter, (((1,), (1,)), ((), ())), preferred_element_type=jnp.float32
    )


def silu_slope(pre_act):
    sigmoid = jax.nn.sigmoid(pre_act)
    return sigmoid * (1.0 + pre_act * (1.0 - sigmoid))


def decoder_forward(features, low_in, low_mid, low_out):
    pre_acts = [matmul(low_in, features)]
    activations = [jax.nn.silu(pre_acts[0]).astype(jnp.bfloat16)]
    pre_acts.append(matmul(low_mid[0], activations[-1]))
    activations.append(jax.nn.silu(pre_acts[-1]).astype(jnp.bfloat16))
    return (matmul(low_out, activations[-1]), pre_acts, activations)


def decoder_backward(features, pre_acts, activations, cotangent, low_in, low_mid, low_out):
    out_cotangent = cotangent.astype(jnp.bfloat16)
    grad_out = contract_cols(out_cotangent, activations[-1])
    upward = contract_rows(low_out, out_cotangent)
    grads_mid = []
    delta_low = (upward * silu_slope(pre_acts[1])).astype(jnp.bfloat16)
    grads_mid.insert(0, contract_cols(delta_low, activations[0]))
    upward = contract_rows(low_mid[0], delta_low)
    delta_low = (upward * silu_slope(pre_acts[0])).astype(jnp.bfloat16)
    grad_in = contract_cols(delta_low, features)
    feature_grad = contract_rows(low_in, delta_low)
    return (grad_in, jnp.stack(grads_mid), grad_out, feature_grad)


def pixel_cotangent(value_error, row_error, row_prior, col_error, col_prior):
    return (
        2.0 * LOSS_VALUE * value_error
        + 2.0 * (row_prior - row_error)
        + 2.0 * (col_prior - col_error)
    )


def clip_factor(total, entries):
    return jnp.minimum(1.0, CLIP_RMS / jnp.sqrt(total / entries + MEAN_EPSILON))


def adam_step(gradient, moment_one, moment_two, clip_scale):
    clipped = gradient * clip_scale
    new_one = BETA_ONE * moment_one + (1.0 - BETA_ONE) * clipped
    new_two = BETA_TWO * moment_two + (1.0 - BETA_TWO) * clipped * clipped
    return (
        new_one
        / (1.0 - BETA_ONE**ADAM_STEP)
        / (jnp.sqrt(new_two / (1.0 - BETA_TWO**ADAM_STEP)) + ADAM_EPSILON)
    )


MESH = pl.DeviceIdType.MESH
LANES = 128
SUBLANES = 8


def sum_kernel(
    mine_ref, sum_ref, from_pair, paired, arrived, own, pair_send, pair_recv, send, recv
):
    row, col = lax.axis_index("row"), lax.axis_index("col")
    chips = mine_ref.shape[1]
    half_cols = lax.axis_size("col") // 2
    core = lax.rem(col, 2)
    chip = row * half_cols + lax.div(col, 2)
    pair = (row, col + 1 - 2 * core)

    def place(step):
        other = lax.rem(chip + step, chips)
        return other, (lax.div(other, half_cols), lax.rem(other, half_cols) * 2 + core)

    def pair_copy(slot, source, target):
        return pltpu.make_async_remote_copy(
            src_ref=source,
            dst_ref=target,
            send_sem=pair_send.at[slot],
            recv_sem=pair_recv.at[slot],
            device_id=pair,
            device_id_type=MESH,
        )

    def block_copy(step):
        other, device = place(step)
        return pltpu.make_async_remote_copy(
            src_ref=paired.at[other],
            dst_ref=arrived.at[step],
            send_sem=send.at[0, step],
            recv_sem=recv.at[0, step],
            device_id=device,
            device_id_type=MESH,
        )

    def result_copy(step):
        _, device = place(step)
        return pltpu.make_async_remote_copy(
            src_ref=own,
            dst_ref=sum_ref.at[core, chip],
            send_sem=send.at[1, step],
            recv_sem=recv.at[1, step],
            device_id=device,
            device_id_type=MESH,
        )

    barrier = pltpu.get_barrier_semaphore()
    pl.semaphore_signal(barrier, inc=1, device_id=pair, device_id_type=MESH)

    @pl.loop(1, chips)
    def _(step):
        _, device = place(step)
        pl.semaphore_signal(barrier, inc=1, device_id=device, device_id_type=MESH)

    pl.semaphore_wait(barrier, chips)

    first = pair_copy(0, mine_ref.at[1 - core], from_pair)
    first.start()
    first.wait()

    @pl.loop(1, chips)
    def _(step):
        other, _ = place(step)
        paired[other] = mine_ref[core, other] + from_pair[other]
        block_copy(step).start()

    own[...] = mine_ref[core, chip] + from_pair[chip]

    @pl.loop(1, chips)
    def _(step):
        block_copy(step).wait()
        own[...] += arrived[step]

    @pl.loop(1, chips)
    def _(step):
        result_copy(step).start()

    sum_ref[core, chip] = own[...]

    @pl.loop(1, chips)
    def _(step):
        result_copy(step).wait()

    last = pair_copy(1, sum_ref.at[core], sum_ref.at[core])
    last.start()
    last.wait()


def sum_over_devices(grad_in, grad_mid, grad_out, grid_local):
    devices = lax.axis_size("row") * lax.axis_size("col")
    chips = devices // 2
    hidden, inputs = grad_in.shape
    outputs = grad_out.shape[0]
    used = hidden + inputs + outputs + 1
    lanes = -(-used // LANES) * LANES
    rows = -(-hidden // (devices * SUBLANES)) * SUBLANES
    total_column = jnp.zeros((hidden, 1), jnp.float32).at[0, 0].set(grid_local)
    packed = jnp.concatenate(
        [
            grad_mid[0],
            grad_in,
            grad_out.T,
            total_column,
            jnp.zeros((hidden, lanes - used), jnp.float32),
        ],
        axis=1,
    )
    packed = jnp.pad(packed, ((0, rows * devices - hidden), (0, 0)))
    shape = (2, chips, rows, lanes)
    summed = pl.pallas_call(
        sum_kernel,
        out_shape=jax.ShapeDtypeStruct(shape, jnp.float32),
        in_specs=[pl.BlockSpec(memory_space=pltpu.VMEM)],
        out_specs=pl.BlockSpec(memory_space=pltpu.VMEM),
        scratch_shapes=[
            pltpu.VMEM(shape[1:], jnp.float32),
            pltpu.VMEM(shape[1:], jnp.float32),
            pltpu.VMEM(shape[1:], jnp.float32),
            pltpu.VMEM(shape[2:], jnp.float32),
            pltpu.SemaphoreType.DMA((2,)),
            pltpu.SemaphoreType.DMA((2,)),
            pltpu.SemaphoreType.DMA((2, chips)),
            pltpu.SemaphoreType.DMA((2, chips)),
        ],
        compiler_params=pltpu.CompilerParams(collective_id=0, has_side_effects=True),
    )(packed.reshape(shape))
    summed = summed.reshape(rows * devices, lanes)[:hidden]
    return (
        summed[:, hidden : hidden + inputs],
        summed[:, :hidden][None],
        summed[:, hidden + inputs : hidden + inputs + outputs].T,
        summed[0, used - 1],
    )


def shards(
    offsets,
    targets,
    grid_fine,
    grid_coarse,
    weight_in,
    weight_mid,
    weight_out,
    fine_first,
    fine_second,
    coarse_first,
    coarse_second,
    in_first,
    in_second,
    mid_first,
    mid_second,
    out_first,
    out_second,
):
    channels, sample_rows, sample_cols = grid_fine.shape
    coarse_rows = grid_coarse.shape[1]
    coarse_cols = grid_coarse.shape[2]
    low_in = weight_in.astype(jnp.bfloat16)
    low_mid = weight_mid.astype(jnp.bfloat16)
    low_out = weight_out.astype(jnp.bfloat16)
    top_rows = jnp.concatenate([grid_fine[:, :1, :], grid_coarse[:, :1, :]], axis=2)
    top_rows = shifted(top_rows, "row", -1)
    fine_tall = jnp.concatenate([grid_fine, top_rows[:, :, :sample_cols]], axis=1)
    coarse_tall = jnp.concatenate([grid_coarse, top_rows[:, :, sample_cols:]], axis=1)
    edge_cols = jnp.concatenate([fine_tall[:, :, :1], coarse_tall[:, :, :1]], axis=1)
    edge_cols = shifted(edge_cols, "col", -1)
    fine_ext = jnp.concatenate([fine_tall, edge_cols[:, : sample_rows + 1, :]], axis=2)
    coarse_ext = jnp.concatenate([coarse_tall, edge_cols[:, sample_rows + 1 :, :]], axis=2)
    tables = level_tables(sample_rows, sample_cols, offsets[0, 0, 0], offsets[0, 0, 1])
    features = sample_features(fine_ext, coarse_ext, tables)
    predicted, pre_acts, activations = decoder_forward(features, low_in, low_mid, low_out)
    outputs = predicted.shape[0]
    predicted = predicted.reshape(outputs, sample_rows, sample_cols)
    below = shifted(predicted[:, :1, :], "row", -1)
    beside = shifted(predicted[:, :, :1], "col", -1)
    row_global = lax.axis_index("row") * sample_rows + jnp.arange(sample_rows, dtype=jnp.int32)
    col_global = lax.axis_index("col") * sample_cols + jnp.arange(sample_cols, dtype=jnp.int32)
    row_valid = (row_global < lax.axis_size("row") * sample_rows - 1)[None, :, None]
    col_valid = (col_global < lax.axis_size("col") * sample_cols - 1)[None, None, :]
    row_next = jnp.concatenate([predicted[:, 1:, :], below], axis=1)
    col_next = jnp.concatenate([predicted[:, :, 1:], beside], axis=2)
    value_error = predicted - targets[0]
    row_error = jnp.where(row_valid, row_next - predicted - targets[1], 0.0)
    col_error = jnp.where(col_valid, col_next - predicted - targets[2], 0.0)
    above = shifted(row_error[:, -1:, :], "row", 1)
    before = shifted(col_error[:, :, -1:], "col", 1)
    row_prior = jnp.concatenate([above, row_error[:, :-1, :]], axis=1)
    col_prior = jnp.concatenate([before, col_error[:, :, :-1]], axis=2)
    cotangent = pixel_cotangent(value_error, row_error, row_prior, col_error, col_prior)
    grad_in, grad_mid, grad_out, feature_grad = decoder_backward(
        features,
        pre_acts,
        activations,
        cotangent.reshape(outputs, sample_rows * sample_cols),
        low_in,
        low_mid,
        low_out,
    )
    fine_back, coarse_back = spread_features(feature_grad, tables)
    side_cols = jnp.concatenate(
        [fine_back[:, :, sample_cols:], coarse_back[:, :, coarse_cols:]], axis=1
    )
    side_cols = shifted(side_cols, "col", 1)
    fine_tall_grad = jnp.concatenate(
        [fine_back[:, :, :1] + side_cols[:, : sample_rows + 1, :], fine_back[:, :, 1:sample_cols]],
        axis=2,
    )
    coarse_tall_grad = jnp.concatenate(
        [
            coarse_back[:, :, :1] + side_cols[:, sample_rows + 1 :, :],
            coarse_back[:, :, 1:coarse_cols],
        ],
        axis=2,
    )
    bottom_rows = jnp.concatenate(
        [fine_tall_grad[:, sample_rows:, :], coarse_tall_grad[:, coarse_rows:, :]], axis=2
    )
    bottom_rows = shifted(bottom_rows, "row", 1)
    fine_grad = jnp.concatenate(
        [
            fine_tall_grad[:, :1, :] + bottom_rows[:, :, :sample_cols],
            fine_tall_grad[:, 1:sample_rows, :],
        ],
        axis=1,
    )
    coarse_grad = jnp.concatenate(
        [
            coarse_tall_grad[:, :1, :] + bottom_rows[:, :, sample_cols:],
            coarse_tall_grad[:, 1:coarse_rows, :],
        ],
        axis=1,
    )
    grid_local = jnp.sum(fine_grad * fine_grad) + jnp.sum(coarse_grad * coarse_grad)
    devices = lax.axis_size("row") * lax.axis_size("col")
    grid_entries = (fine_grad.size + coarse_grad.size) * devices
    decoder_entries = weight_in.size + weight_mid.size + weight_out.size
    grad_in, grad_mid, grad_out, grid_total = sum_over_devices(
        grad_in, grad_mid, grad_out, grid_local
    )
    decoder_total = (
        jnp.sum(grad_in * grad_in) + jnp.sum(grad_mid * grad_mid) + jnp.sum(grad_out * grad_out)
    )
    decoder_scale = clip_factor(decoder_total, decoder_entries)
    middle_step = adam_step(grad_mid, mid_first, mid_second, decoder_scale)
    grid_scale = clip_factor(grid_total, grid_entries)
    fine_step = adam_step(fine_grad, fine_first, fine_second, grid_scale)
    coarse_step = adam_step(coarse_grad, coarse_first, coarse_second, grid_scale)
    input_step = adam_step(grad_in, in_first, in_second, decoder_scale)
    output_step = adam_step(grad_out, out_first, out_second, decoder_scale)
    return (fine_step, coarse_step, input_step, middle_step, output_step)


def solution(mesh):
    placed = (
        P("row", "col", None),
        P(None, None, "row", "col"),
        P(None, "row", "col"),
        P(None, "row", "col"),
        P(),
        P(),
        P(),
        P(None, "row", "col"),
        P(None, "row", "col"),
        P(None, "row", "col"),
        P(None, "row", "col"),
        P(),
        P(),
        P(),
        P(),
        P(),
        P(),
    )
    return jax.shard_map(
        shards,
        mesh=mesh,
        in_specs=placed,
        out_specs=(P(None, "row", "col"), P(None, "row", "col"), P(), P(), P()),
        check_vma=False,
    )
```

```python
import functools

import jax
import jax.numpy as jnp
from jax import lax
from jax.experimental import pallas as pl
from jax.experimental.pallas import tpu as pltpu
from jax.sharding import PartitionSpec as P

SUB = 4
RATIO = 4
ADAM_STEP = 10


BETA_ONE = 0.9
BETA_TWO = 0.99
ADAM_EPSILON = 1e-08
CLIP_RMS = 0.01
LOSS_VALUE = 0.25
MEAN_EPSILON = 1e-06


def shifted(block, axis, distance):
    devices = range(lax.axis_size(axis))
    route = [(i - distance, i) for i in devices if i - distance in devices]
    return lax.ppermute(block, axis, route)


def interp_table(samples, level_ratio, offset):
    positions = jnp.arange(samples, dtype=jnp.int32)
    base_index = positions // level_ratio
    fraction = (
        (positions % level_ratio).astype(jnp.float32) + offset.astype(jnp.float32) / SUB
    ) / level_ratio
    column = jnp.arange(samples // level_ratio + 1, dtype=jnp.int32)
    lower_hit = (column[None, :] == base_index[:, None]).astype(jnp.float32)
    upper_hit = (column[None, :] == base_index[:, None] + 1).astype(jnp.float32)
    return lower_hit * (1.0 - fraction)[:, None] + upper_hit * fraction[:, None]


def level_tables(row_count, col_count, shift_y, shift_x):
    return (
        interp_table(row_count, 1, shift_y),
        interp_table(col_count, 1, shift_x),
        interp_table(row_count, RATIO, shift_y),
        interp_table(col_count, RATIO, shift_x),
    )


def sample_level(extended, row_table, col_table):
    across = jnp.einsum("kjl,ml->kjm", extended, col_table, precision=lax.Precision.HIGHEST)
    return jnp.einsum("ij,kjm->kim", row_table, across, precision=lax.Precision.HIGHEST)


def spread_level(cotangent, row_table, col_table):
    backward = jnp.einsum("ij,kim->kjm", row_table, cotangent, precision=lax.Precision.HIGHEST)
    return jnp.einsum("kjm,ml->kjl", backward, col_table, precision=lax.Precision.HIGHEST)


def sample_features(fine_ext, coarse_ext, tables):
    fine_feat = sample_level(fine_ext, tables[0], tables[1])
    coarse_feat = sample_level(coarse_ext, tables[2], tables[3])
    channels, row_count, col_count = fine_feat.shape
    return jnp.concatenate(
        [
            fine_feat.reshape(channels, row_count * col_count),
            coarse_feat.reshape(channels, row_count * col_count),
        ],
        axis=0,
    ).astype(jnp.bfloat16)


def spread_features(feature_grad, tables):
    channels = feature_grad.shape[0] // 2
    row_count = tables[0].shape[0]
    col_count = tables[1].shape[0]
    fine_cot = feature_grad[:channels].reshape(channels, row_count, col_count)
    coarse_cot = feature_grad[channels:].reshape(channels, row_count, col_count)
    return (
        spread_level(fine_cot, tables[0], tables[1]),
        spread_level(coarse_cot, tables[2], tables[3]),
    )


def matmul(former, latter):
    return jnp.dot(former, latter, preferred_element_type=jnp.float32)


def contract_rows(former, latter):
    return lax.dot_general(
        former, latter, (((0,), (0,)), ((), ())), preferred_element_type=jnp.float32
    )


def contract_cols(former, latter):
    return lax.dot_general(
        former, latter, (((1,), (1,)), ((), ())), preferred_element_type=jnp.float32
    )


def silu_slope(pre_act):
    sigmoid = jax.nn.sigmoid(pre_act)
    return sigmoid * (1.0 + pre_act * (1.0 - sigmoid))


def decoder_forward(features, low_in, low_mid, low_out):
    pre_acts = [matmul(low_in, features)]
    activations = [jax.nn.silu(pre_acts[0]).astype(jnp.bfloat16)]
    pre_acts.append(matmul(low_mid[0], activations[-1]))
    activations.append(jax.nn.silu(pre_acts[-1]).astype(jnp.bfloat16))
    return (matmul(low_out, activations[-1]), pre_acts, activations)


def decoder_backward(features, pre_acts, activations, cotangent, low_in, low_mid, low_out):
    out_cotangent = cotangent.astype(jnp.bfloat16)
    grad_out = contract_cols(out_cotangent, activations[-1])
    upward = contract_rows(low_out, out_cotangent)
    grads_mid = []
    delta_low = (upward * silu_slope(pre_acts[1])).astype(jnp.bfloat16)
    grads_mid.insert(0, contract_cols(delta_low, activations[0]))
    upward = contract_rows(low_mid[0], delta_low)
    delta_low = (upward * silu_slope(pre_acts[0])).astype(jnp.bfloat16)
    grad_in = contract_cols(delta_low, features)
    feature_grad = contract_rows(low_in, delta_low)
    return (grad_in, jnp.stack(grads_mid), grad_out, feature_grad)


def pixel_cotangent(value_error, row_error, row_prior, col_error, col_prior):
    return (
        2.0 * LOSS_VALUE * value_error
        + 2.0 * (row_prior - row_error)
        + 2.0 * (col_prior - col_error)
    )


def clip_factor(total, entries):
    return jnp.minimum(1.0, CLIP_RMS / jnp.sqrt(total / entries + MEAN_EPSILON))


def adam_step(gradient, moment_one, moment_two, clip_scale):
    clipped = gradient * clip_scale
    new_one = BETA_ONE * moment_one + (1.0 - BETA_ONE) * clipped
    new_two = BETA_TWO * moment_two + (1.0 - BETA_TWO) * clipped * clipped
    return (
        new_one
        / (1.0 - BETA_ONE**ADAM_STEP)
        / (jnp.sqrt(new_two / (1.0 - BETA_TWO**ADAM_STEP)) + ADAM_EPSILON)
    )


MESH = pl.DeviceIdType.MESH
LANES = 128
SUBLANES = 8


def decoder_kernel(
    used,
    mid_ref,
    rest_ref,
    mid_first_ref,
    mid_second_ref,
    rest_first_ref,
    rest_second_ref,
    mid_step_ref,
    rest_step_ref,
    total_ref,
    mine_ref,
    sum_ref,
    from_pair,
    paired,
    arrived,
    own,
    pair_send,
    pair_recv,
    send,
    recv,
):
    row, col = lax.axis_index("row"), lax.axis_index("col")
    chips = mine_ref.shape[1]
    half_cols = lax.axis_size("col") // 2
    core = lax.rem(col, 2)
    chip = row * half_cols + lax.div(col, 2)
    pair = (row, col + 1 - 2 * core)

    def place(step):
        other = lax.rem(chip + step, chips)
        return other, (lax.div(other, half_cols), lax.rem(other, half_cols) * 2 + core)

    def pair_copy(slot, source, target):
        return pltpu.make_async_remote_copy(
            src_ref=source,
            dst_ref=target,
            send_sem=pair_send.at[slot],
            recv_sem=pair_recv.at[slot],
            device_id=pair,
            device_id_type=MESH,
        )

    def block_copy(step):
        other, device = place(step)
        return pltpu.make_async_remote_copy(
            src_ref=paired.at[other],
            dst_ref=arrived.at[step],
            send_sem=send.at[0, step],
            recv_sem=recv.at[0, step],
            device_id=device,
            device_id_type=MESH,
        )

    def result_copy(step):
        _, device = place(step)
        return pltpu.make_async_remote_copy(
            src_ref=own,
            dst_ref=sum_ref.at[core, chip],
            send_sem=send.at[1, step],
            recv_sem=recv.at[1, step],
            device_id=device,
            device_id_type=MESH,
        )

    barrier = pltpu.get_barrier_semaphore()
    pl.semaphore_signal(barrier, inc=1, device_id=pair, device_id_type=MESH)

    @pl.loop(1, chips)
    def _(step):
        _, device = place(step)
        pl.semaphore_signal(barrier, inc=1, device_id=device, device_id_type=MESH)

    hidden, mids = mid_ref.shape
    rows, lanes = mine_ref.shape[2:]
    rests = lanes - mids
    blocks = hidden // rows
    for block in range(2 * chips):
        where = divmod(block, chips)
        if block < blocks:
            span = slice(block * rows, (block + 1) * rows)
            mine_ref[where[0], where[1], :, :mids] = mid_ref[span, :]
            mine_ref[where[0], where[1], :, mids:] = rest_ref[span, :]
        else:
            mine_ref[where[0], where[1]] = jnp.zeros((rows, lanes), jnp.float32)

    pl.semaphore_wait(barrier, chips)

    first = pair_copy(0, mine_ref.at[1 - core], from_pair)
    first.start()
    first.wait()

    @pl.loop(1, chips)
    def _(step):
        other, _ = place(step)
        paired[other] = mine_ref[core, other] + from_pair[other]
        block_copy(step).start()

    own[...] = mine_ref[core, chip] + from_pair[chip]

    @pl.loop(1, chips)
    def _(step):
        block_copy(step).wait()
        own[...] += arrived[step]

    @pl.loop(1, chips)
    def _(step):
        result_copy(step).start()

    sum_ref[core, chip] = own[...]

    @pl.loop(1, chips)
    def _(step):
        result_copy(step).wait()

    last = pair_copy(1, sum_ref.at[core], sum_ref.at[core])
    last.start()
    last.wait()

    total_ref[...] = sum_ref[0, 0, :SUBLANES, mids:]
    kept = lax.broadcasted_iota(jnp.int32, (rows, rests), 1) < used
    mid_squares = jnp.zeros((rows, mids), jnp.float32)
    rest_squares = jnp.zeros((rows, rests), jnp.float32)
    for block in range(blocks):
        where = divmod(block, chips)
        mid = sum_ref[where[0], where[1], :, :mids]
        rest = sum_ref[where[0], where[1], :, mids:]
        mid_squares += mid * mid
        rest_squares += jnp.where(kept, rest * rest, 0.0)
    total = jnp.sum(mid_squares, keepdims=True) + jnp.sum(rest_squares, keepdims=True)
    scale = clip_factor(total, hidden * (mids + used))
    for block in range(blocks):
        where = divmod(block, chips)
        span = slice(block * rows, (block + 1) * rows)
        mid_step_ref[span, :] = adam_step(
            sum_ref[where[0], where[1], :, :mids],
            mid_first_ref[span, :],
            mid_second_ref[span, :],
            scale,
        )
        rest_step_ref[span, :] = adam_step(
            sum_ref[where[0], where[1], :, mids:],
            rest_first_ref[span, :],
            rest_second_ref[span, :],
            scale,
        )


def decoder_steps(gradients, firsts, seconds, grid_local):
    grad_in, grad_mid, grad_out = gradients
    devices = lax.axis_size("row") * lax.axis_size("col")
    chips = devices // 2
    hidden, inputs = grad_in.shape
    outputs = grad_out.shape[0]
    mids = grad_mid.shape[2]
    used = inputs + outputs
    rests = -(-(used + 1) // LANES) * LANES
    rows = -(-hidden // (devices * SUBLANES)) * SUBLANES

    def beside(block_in, block_out, fill):
        column = jnp.full((hidden, rests - used), fill, jnp.float32)
        return jnp.concatenate([block_in, block_out.T, column], axis=1)

    shape = (2, chips, rows, mids + rests)
    flat = jax.ShapeDtypeStruct((hidden, mids), jnp.float32)
    side = jax.ShapeDtypeStruct((hidden, rests), jnp.float32)
    mid_step, rest_step, total = pl.pallas_call(
        functools.partial(decoder_kernel, used),
        out_shape=(flat, side, jax.ShapeDtypeStruct((SUBLANES, rests), jnp.float32)),
        in_specs=[pl.BlockSpec(memory_space=pltpu.VMEM)] * 6,
        out_specs=(pl.BlockSpec(memory_space=pltpu.VMEM),) * 3,
        scratch_shapes=[
            pltpu.VMEM(shape, jnp.float32),
            pltpu.VMEM(shape, jnp.float32),
            pltpu.VMEM(shape[1:], jnp.float32),
            pltpu.VMEM(shape[1:], jnp.float32),
            pltpu.VMEM(shape[1:], jnp.float32),
            pltpu.VMEM(shape[2:], jnp.float32),
            pltpu.SemaphoreType.DMA((2,)),
            pltpu.SemaphoreType.DMA((2,)),
            pltpu.SemaphoreType.DMA((2, chips)),
            pltpu.SemaphoreType.DMA((2, chips)),
        ],
        compiler_params=pltpu.CompilerParams(collective_id=0, has_side_effects=True),
    )(
        grad_mid[0],
        beside(grad_in, grad_out, grid_local),
        firsts[1][0],
        seconds[1][0],
        beside(firsts[0], firsts[2], 0.0),
        beside(seconds[0], seconds[2], 1.0),
    )
    return (
        rest_step[:, :inputs],
        mid_step[None],
        rest_step[:, inputs:used].T,
        total[0, used],
    )


def shards(
    offsets,
    targets,
    grid_fine,
    grid_coarse,
    weight_in,
    weight_mid,
    weight_out,
    fine_first,
    fine_second,
    coarse_first,
    coarse_second,
    in_first,
    in_second,
    mid_first,
    mid_second,
    out_first,
    out_second,
):
    channels, sample_rows, sample_cols = grid_fine.shape
    coarse_rows = grid_coarse.shape[1]
    coarse_cols = grid_coarse.shape[2]
    low_in = weight_in.astype(jnp.bfloat16)
    low_mid = weight_mid.astype(jnp.bfloat16)
    low_out = weight_out.astype(jnp.bfloat16)
    top_rows = jnp.concatenate([grid_fine[:, :1, :], grid_coarse[:, :1, :]], axis=2)
    top_rows = shifted(top_rows, "row", -1)
    fine_tall = jnp.concatenate([grid_fine, top_rows[:, :, :sample_cols]], axis=1)
    coarse_tall = jnp.concatenate([grid_coarse, top_rows[:, :, sample_cols:]], axis=1)
    edge_cols = jnp.concatenate([fine_tall[:, :, :1], coarse_tall[:, :, :1]], axis=1)
    edge_cols = shifted(edge_cols, "col", -1)
    fine_ext = jnp.concatenate([fine_tall, edge_cols[:, : sample_rows + 1, :]], axis=2)
    coarse_ext = jnp.concatenate([coarse_tall, edge_cols[:, sample_rows + 1 :, :]], axis=2)
    tables = level_tables(sample_rows, sample_cols, offsets[0, 0, 0], offsets[0, 0, 1])
    features = sample_features(fine_ext, coarse_ext, tables)
    predicted, pre_acts, activations = decoder_forward(features, low_in, low_mid, low_out)
    outputs = predicted.shape[0]
    predicted = predicted.reshape(outputs, sample_rows, sample_cols)
    below = shifted(predicted[:, :1, :], "row", -1)
    beside = shifted(predicted[:, :, :1], "col", -1)
    above = jnp.concatenate([predicted[:, -1:, :], targets[1][:, -1:, :]], axis=0)
    above = shifted(above, "row", 1)
    before = jnp.concatenate([predicted[:, :, -1:], targets[2][:, :, -1:]], axis=0)
    before = shifted(before, "col", 1)
    row_global = lax.axis_index("row") * sample_rows + jnp.arange(sample_rows, dtype=jnp.int32)
    col_global = lax.axis_index("col") * sample_cols + jnp.arange(sample_cols, dtype=jnp.int32)
    row_valid = (row_global < lax.axis_size("row") * sample_rows - 1)[None, :, None]
    col_valid = (col_global < lax.axis_size("col") * sample_cols - 1)[None, None, :]
    row_next = jnp.concatenate([predicted[:, 1:, :], below], axis=1)
    col_next = jnp.concatenate([predicted[:, :, 1:], beside], axis=2)
    value_error = predicted - targets[0]
    row_error = jnp.where(row_valid, row_next - predicted - targets[1], 0.0)
    col_error = jnp.where(col_valid, col_next - predicted - targets[2], 0.0)
    above = jnp.where(
        lax.axis_index("row") > 0, predicted[:, :1, :] - above[:outputs] - above[outputs:], 0.0
    )
    before = jnp.where(
        lax.axis_index("col") > 0, predicted[:, :, :1] - before[:outputs] - before[outputs:], 0.0
    )
    row_prior = jnp.concatenate([above, row_error[:, :-1, :]], axis=1)
    col_prior = jnp.concatenate([before, col_error[:, :, :-1]], axis=2)
    cotangent = pixel_cotangent(value_error, row_error, row_prior, col_error, col_prior)
    grad_in, grad_mid, grad_out, feature_grad = decoder_backward(
        features,
        pre_acts,
        activations,
        cotangent.reshape(outputs, sample_rows * sample_cols),
        low_in,
        low_mid,
        low_out,
    )
    fine_back, coarse_back = spread_features(feature_grad, tables)
    side_cols = jnp.concatenate(
        [fine_back[:, :, sample_cols:], coarse_back[:, :, coarse_cols:]], axis=1
    )
    side_cols = shifted(side_cols, "col", 1)
    fine_tall_grad = jnp.concatenate(
        [fine_back[:, :, :1] + side_cols[:, : sample_rows + 1, :], fine_back[:, :, 1:sample_cols]],
        axis=2,
    )
    coarse_tall_grad = jnp.concatenate(
        [
            coarse_back[:, :, :1] + side_cols[:, sample_rows + 1 :, :],
            coarse_back[:, :, 1:coarse_cols],
        ],
        axis=2,
    )
    bottom_rows = jnp.concatenate(
        [fine_tall_grad[:, sample_rows:, :], coarse_tall_grad[:, coarse_rows:, :]], axis=2
    )
    bottom_rows = shifted(bottom_rows, "row", 1)
    fine_grad = jnp.concatenate(
        [
            fine_tall_grad[:, :1, :] + bottom_rows[:, :, :sample_cols],
            fine_tall_grad[:, 1:sample_rows, :],
        ],
        axis=1,
    )
    coarse_grad = jnp.concatenate(
        [
            coarse_tall_grad[:, :1, :] + bottom_rows[:, :, sample_cols:],
            coarse_tall_grad[:, 1:coarse_rows, :],
        ],
        axis=1,
    )
    grid_local = jnp.sum(fine_grad * fine_grad) + jnp.sum(coarse_grad * coarse_grad)
    devices = lax.axis_size("row") * lax.axis_size("col")
    grid_entries = (fine_grad.size + coarse_grad.size) * devices
    input_step, middle_step, output_step, grid_total = decoder_steps(
        (grad_in, grad_mid, grad_out),
        (in_first, mid_first, out_first),
        (in_second, mid_second, out_second),
        grid_local,
    )
    grid_scale = clip_factor(grid_total, grid_entries)
    fine_step = adam_step(fine_grad, fine_first, fine_second, grid_scale)
    coarse_step = adam_step(coarse_grad, coarse_first, coarse_second, grid_scale)
    return (fine_step, coarse_step, input_step, middle_step, output_step)


def solution(mesh):
    placed = (
        P("row", "col", None),
        P(None, None, "row", "col"),
        P(None, "row", "col"),
        P(None, "row", "col"),
        P(),
        P(),
        P(),
        P(None, "row", "col"),
        P(None, "row", "col"),
        P(None, "row", "col"),
        P(None, "row", "col"),
        P(),
        P(),
        P(),
        P(),
        P(),
        P(),
    )
    return jax.shard_map(
        shards,
        mesh=mesh,
        in_specs=placed,
        out_specs=(P(None, "row", "col"), P(None, "row", "col"), P(), P(), P()),
        check_vma=False,
    )
```

```python
import functools

import jax
import jax.numpy as jnp
from jax import lax
from jax.experimental import pallas as pl
from jax.experimental.pallas import tpu as pltpu
from jax.sharding import PartitionSpec as P

SUB = 4
RATIO = 4
ADAM_STEP = 10


BETA_ONE = 0.9
BETA_TWO = 0.99
ADAM_EPSILON = 1e-08
CLIP_RMS = 0.01
LOSS_VALUE = 0.25
MEAN_EPSILON = 1e-06


def shifted(block, axis, distance):
    devices = range(lax.axis_size(axis))
    route = [(i - distance, i) for i in devices if i - distance in devices]
    return lax.ppermute(block, axis, route)


def interp_table(samples, level_ratio, offset):
    positions = jnp.arange(samples, dtype=jnp.int32)
    base_index = positions // level_ratio
    fraction = (
        (positions % level_ratio).astype(jnp.float32) + offset.astype(jnp.float32) / SUB
    ) / level_ratio
    column = jnp.arange(samples // level_ratio + 1, dtype=jnp.int32)
    lower_hit = (column[None, :] == base_index[:, None]).astype(jnp.float32)
    upper_hit = (column[None, :] == base_index[:, None] + 1).astype(jnp.float32)
    return lower_hit * (1.0 - fraction)[:, None] + upper_hit * fraction[:, None]


def level_tables(row_count, col_count, shift_y, shift_x):
    return (
        interp_table(row_count, 1, shift_y),
        interp_table(col_count, 1, shift_x),
        interp_table(row_count, RATIO, shift_y),
        interp_table(col_count, RATIO, shift_x),
    )


def sample_level(extended, row_table, col_table):
    across = jnp.einsum("kjl,ml->kjm", extended, col_table, precision=lax.Precision.HIGHEST)
    return jnp.einsum("ij,kjm->kim", row_table, across, precision=lax.Precision.HIGHEST)


def spread_level(cotangent, row_table, col_table):
    backward = jnp.einsum("ij,kim->kjm", row_table, cotangent, precision=lax.Precision.HIGHEST)
    return jnp.einsum("kjm,ml->kjl", backward, col_table, precision=lax.Precision.HIGHEST)


def sample_features(fine_ext, coarse_ext, tables):
    fine_feat = sample_level(fine_ext, tables[0], tables[1])
    coarse_feat = sample_level(coarse_ext, tables[2], tables[3])
    channels, row_count, col_count = fine_feat.shape
    return jnp.concatenate(
        [
            fine_feat.reshape(channels, row_count * col_count),
            coarse_feat.reshape(channels, row_count * col_count),
        ],
        axis=0,
    ).astype(jnp.bfloat16)


def spread_features(feature_grad, tables):
    channels = feature_grad.shape[0] // 2
    row_count = tables[0].shape[0]
    col_count = tables[1].shape[0]
    fine_cot = feature_grad[:channels].reshape(channels, row_count, col_count)
    coarse_cot = feature_grad[channels:].reshape(channels, row_count, col_count)
    return (
        spread_level(fine_cot, tables[0], tables[1]),
        spread_level(coarse_cot, tables[2], tables[3]),
    )


def matmul(former, latter):
    return jnp.dot(former, latter, preferred_element_type=jnp.float32)


def contract_rows(former, latter):
    return lax.dot_general(
        former, latter, (((0,), (0,)), ((), ())), preferred_element_type=jnp.float32
    )


def contract_cols(former, latter):
    return lax.dot_general(
        former, latter, (((1,), (1,)), ((), ())), preferred_element_type=jnp.float32
    )


def silu_slope(pre_act):
    sigmoid = jax.nn.sigmoid(pre_act)
    return sigmoid * (1.0 + pre_act * (1.0 - sigmoid))


def decoder_forward(features, low_in, low_mid, low_out):
    pre_acts = [matmul(low_in, features)]
    activations = [jax.nn.silu(pre_acts[0]).astype(jnp.bfloat16)]
    pre_acts.append(matmul(low_mid[0], activations[-1]))
    activations.append(jax.nn.silu(pre_acts[-1]).astype(jnp.bfloat16))
    return (matmul(low_out, activations[-1]), pre_acts, activations)


def decoder_backward(features, pre_acts, activations, cotangent, low_in, low_mid, low_out):
    out_cotangent = cotangent.astype(jnp.bfloat16)
    grad_out = contract_cols(out_cotangent, activations[-1])
    upward = contract_rows(low_out, out_cotangent)
    grads_mid = []
    delta_low = (upward * silu_slope(pre_acts[1])).astype(jnp.bfloat16)
    grads_mid.insert(0, contract_cols(delta_low, activations[0]))
    upward = contract_rows(low_mid[0], delta_low)
    delta_low = (upward * silu_slope(pre_acts[0])).astype(jnp.bfloat16)
    grad_in = contract_cols(delta_low, features)
    feature_grad = contract_rows(low_in, delta_low)
    return (grad_in, jnp.stack(grads_mid), grad_out, feature_grad)


def pixel_cotangent(value_error, row_error, row_prior, col_error, col_prior):
    return (
        2.0 * LOSS_VALUE * value_error
        + 2.0 * (row_prior - row_error)
        + 2.0 * (col_prior - col_error)
    )


def clip_factor(total, entries):
    return jnp.minimum(1.0, CLIP_RMS / jnp.sqrt(total / entries + MEAN_EPSILON))


def adam_step(gradient, moment_one, moment_two, clip_scale):
    clipped = gradient * clip_scale
    new_one = BETA_ONE * moment_one + (1.0 - BETA_ONE) * clipped
    new_two = BETA_TWO * moment_two + (1.0 - BETA_TWO) * clipped * clipped
    return (
        new_one
        / (1.0 - BETA_ONE**ADAM_STEP)
        / (jnp.sqrt(new_two / (1.0 - BETA_TWO**ADAM_STEP)) + ADAM_EPSILON)
    )


MESH = pl.DeviceIdType.MESH
LANES = 128
SUBLANES = 8


def decoder_kernel(
    used,
    mid_ref,
    rest_ref,
    mid_first_hbm,
    mid_second_hbm,
    rest_first_ref,
    rest_second_ref,
    mid_step_ref,
    rest_step_ref,
    total_ref,
    mine_ref,
    sum_ref,
    from_pair,
    paired,
    arrived,
    own,
    pair_send,
    pair_recv,
    send,
    recv,
    mid_first_ref,
    mid_second_ref,
    load_sem,
):
    row, col = lax.axis_index("row"), lax.axis_index("col")
    chips = mine_ref.shape[1]
    half_cols = lax.axis_size("col") // 2
    core = lax.rem(col, 2)
    chip = row * half_cols + lax.div(col, 2)
    pair = (row, col + 1 - 2 * core)

    def place(step):
        other = lax.rem(chip + step, chips)
        return other, (lax.div(other, half_cols), lax.rem(other, half_cols) * 2 + core)

    def pair_copy(slot, source, target):
        return pltpu.make_async_remote_copy(
            src_ref=source,
            dst_ref=target,
            send_sem=pair_send.at[slot],
            recv_sem=pair_recv.at[slot],
            device_id=pair,
            device_id_type=MESH,
        )

    def block_copy(step):
        other, device = place(step)
        return pltpu.make_async_remote_copy(
            src_ref=paired.at[other],
            dst_ref=arrived.at[step],
            send_sem=send.at[0, step],
            recv_sem=recv.at[0, step],
            device_id=device,
            device_id_type=MESH,
        )

    def result_copy(step):
        _, device = place(step)
        return pltpu.make_async_remote_copy(
            src_ref=own,
            dst_ref=sum_ref.at[core, chip],
            send_sem=send.at[1, step],
            recv_sem=recv.at[1, step],
            device_id=device,
            device_id_type=MESH,
        )

    barrier = pltpu.get_barrier_semaphore()
    pl.semaphore_signal(barrier, inc=1, device_id=pair, device_id_type=MESH)

    @pl.loop(1, chips)
    def _(step):
        _, device = place(step)
        pl.semaphore_signal(barrier, inc=1, device_id=device, device_id_type=MESH)

    loads = (
        pltpu.make_async_copy(mid_first_hbm, mid_first_ref, load_sem.at[0]),
        pltpu.make_async_copy(mid_second_hbm, mid_second_ref, load_sem.at[1]),
    )
    for load in loads:
        load.start()
    hidden, mids = mid_ref.shape
    rows, lanes = mine_ref.shape[2:]
    rests = lanes - mids
    blocks = hidden // rows
    for block in range(2 * chips):
        where = divmod(block, chips)
        if block < blocks:
            span = slice(block * rows, (block + 1) * rows)
            mine_ref[where[0], where[1], :, :mids] = mid_ref[span, :]
            mine_ref[where[0], where[1], :, mids:] = rest_ref[span, :]
        else:
            mine_ref[where[0], where[1]] = jnp.zeros((rows, lanes), jnp.float32)

    pl.semaphore_wait(barrier, chips)

    first = pair_copy(0, mine_ref.at[1 - core], from_pair)
    first.start()
    first.wait()

    @pl.loop(1, chips)
    def _(step):
        other, _ = place(step)
        paired[other] = mine_ref[core, other] + from_pair[other]
        block_copy(step).start()

    own[...] = mine_ref[core, chip] + from_pair[chip]

    @pl.loop(1, chips)
    def _(step):
        block_copy(step).wait()
        own[...] += arrived[step]

    @pl.loop(1, chips)
    def _(step):
        result_copy(step).start()

    sum_ref[core, chip] = own[...]

    @pl.loop(1, chips)
    def _(step):
        result_copy(step).wait()

    last = pair_copy(1, sum_ref.at[core], sum_ref.at[core])
    last.start()
    last.wait()

    for load in loads:
        load.wait()
    total_ref[...] = sum_ref[0, 0, :SUBLANES, mids:]
    kept = lax.broadcasted_iota(jnp.int32, (rows, rests), 1) < used
    mid_squares = jnp.zeros((rows, mids), jnp.float32)
    rest_squares = jnp.zeros((rows, rests), jnp.float32)
    for block in range(blocks):
        where = divmod(block, chips)
        mid = sum_ref[where[0], where[1], :, :mids]
        rest = sum_ref[where[0], where[1], :, mids:]
        mid_squares += mid * mid
        rest_squares += jnp.where(kept, rest * rest, 0.0)
    total = jnp.sum(mid_squares, keepdims=True) + jnp.sum(rest_squares, keepdims=True)
    scale = clip_factor(total, hidden * (mids + used))
    for block in range(blocks):
        where = divmod(block, chips)
        span = slice(block * rows, (block + 1) * rows)
        mid_step_ref[span, :] = adam_step(
            sum_ref[where[0], where[1], :, :mids],
            mid_first_ref[span, :],
            mid_second_ref[span, :],
            scale,
        )
        rest_step_ref[span, :] = adam_step(
            sum_ref[where[0], where[1], :, mids:],
            rest_first_ref[span, :],
            rest_second_ref[span, :],
            scale,
        )


def decoder_steps(gradients, firsts, seconds, grid_local):
    grad_in, grad_mid, grad_out = gradients
    devices = lax.axis_size("row") * lax.axis_size("col")
    chips = devices // 2
    hidden, inputs = grad_in.shape
    outputs = grad_out.shape[0]
    mids = grad_mid.shape[2]
    used = inputs + outputs
    rests = -(-(used + 1) // LANES) * LANES
    rows = -(-hidden // (devices * SUBLANES)) * SUBLANES

    def beside(block_in, block_out, fill):
        column = jnp.full((hidden, rests - used), fill, jnp.float32)
        return jnp.concatenate([block_in, block_out.T, column], axis=1)

    shape = (2, chips, rows, mids + rests)
    flat = jax.ShapeDtypeStruct((hidden, mids), jnp.float32)
    side = jax.ShapeDtypeStruct((hidden, rests), jnp.float32)
    mid_step, rest_step, total = pl.pallas_call(
        functools.partial(decoder_kernel, used),
        out_shape=(flat, side, jax.ShapeDtypeStruct((SUBLANES, rests), jnp.float32)),
        in_specs=[
            pl.BlockSpec(memory_space=pl.ANY if place in (2, 3) else pltpu.VMEM) for place in range(6)
        ],
        out_specs=(pl.BlockSpec(memory_space=pltpu.VMEM),) * 3,
        scratch_shapes=[
            pltpu.VMEM(shape, jnp.float32),
            pltpu.VMEM(shape, jnp.float32),
            pltpu.VMEM(shape[1:], jnp.float32),
            pltpu.VMEM(shape[1:], jnp.float32),
            pltpu.VMEM(shape[1:], jnp.float32),
            pltpu.VMEM(shape[2:], jnp.float32),
            pltpu.SemaphoreType.DMA((2,)),
            pltpu.SemaphoreType.DMA((2,)),
            pltpu.SemaphoreType.DMA((2, chips)),
            pltpu.SemaphoreType.DMA((2, chips)),
            pltpu.VMEM((hidden, mids), jnp.float32),
            pltpu.VMEM((hidden, mids), jnp.float32),
            pltpu.SemaphoreType.DMA((2,)),
        ],
        compiler_params=pltpu.CompilerParams(collective_id=0, has_side_effects=True),
    )(
        grad_mid[0],
        beside(grad_in, grad_out, grid_local),
        firsts[1][0],
        seconds[1][0],
        beside(firsts[0], firsts[2], 0.0),
        beside(seconds[0], seconds[2], 1.0),
    )
    return (
        rest_step[:, :inputs],
        mid_step[None],
        rest_step[:, inputs:used].T,
        total[0, used],
    )


def shards(
    offsets,
    targets,
    grid_fine,
    grid_coarse,
    weight_in,
    weight_mid,
    weight_out,
    fine_first,
    fine_second,
    coarse_first,
    coarse_second,
    in_first,
    in_second,
    mid_first,
    mid_second,
    out_first,
    out_second,
):
    channels, sample_rows, sample_cols = grid_fine.shape
    coarse_rows = grid_coarse.shape[1]
    coarse_cols = grid_coarse.shape[2]
    low_in = weight_in.astype(jnp.bfloat16)
    low_mid = weight_mid.astype(jnp.bfloat16)
    low_out = weight_out.astype(jnp.bfloat16)
    top_rows = jnp.concatenate([grid_fine[:, :1, :], grid_coarse[:, :1, :]], axis=2)
    top_rows = shifted(top_rows, "row", -1)
    fine_tall = jnp.concatenate([grid_fine, top_rows[:, :, :sample_cols]], axis=1)
    coarse_tall = jnp.concatenate([grid_coarse, top_rows[:, :, sample_cols:]], axis=1)
    edge_cols = jnp.concatenate([fine_tall[:, :, :1], coarse_tall[:, :, :1]], axis=1)
    edge_cols = shifted(edge_cols, "col", -1)
    fine_ext = jnp.concatenate([fine_tall, edge_cols[:, : sample_rows + 1, :]], axis=2)
    coarse_ext = jnp.concatenate([coarse_tall, edge_cols[:, sample_rows + 1 :, :]], axis=2)
    tables = level_tables(sample_rows, sample_cols, offsets[0, 0, 0], offsets[0, 0, 1])
    features = sample_features(fine_ext, coarse_ext, tables)
    predicted, pre_acts, activations = decoder_forward(features, low_in, low_mid, low_out)
    outputs = predicted.shape[0]
    predicted = predicted.reshape(outputs, sample_rows, sample_cols)
    below = shifted(predicted[:, :1, :], "row", -1)
    beside = shifted(predicted[:, :, :1], "col", -1)
    above = jnp.concatenate([predicted[:, -1:, :], targets[1][:, -1:, :]], axis=0)
    above = shifted(above, "row", 1)
    before = jnp.concatenate([predicted[:, :, -1:], targets[2][:, :, -1:]], axis=0)
    before = shifted(before, "col", 1)
    row_global = lax.axis_index("row") * sample_rows + jnp.arange(sample_rows, dtype=jnp.int32)
    col_global = lax.axis_index("col") * sample_cols + jnp.arange(sample_cols, dtype=jnp.int32)
    row_valid = (row_global < lax.axis_size("row") * sample_rows - 1)[None, :, None]
    col_valid = (col_global < lax.axis_size("col") * sample_cols - 1)[None, None, :]
    row_next = jnp.concatenate([predicted[:, 1:, :], below], axis=1)
    col_next = jnp.concatenate([predicted[:, :, 1:], beside], axis=2)
    value_error = predicted - targets[0]
    row_error = jnp.where(row_valid, row_next - predicted - targets[1], 0.0)
    col_error = jnp.where(col_valid, col_next - predicted - targets[2], 0.0)
    above = jnp.where(
        lax.axis_index("row") > 0, predicted[:, :1, :] - above[:outputs] - above[outputs:], 0.0
    )
    before = jnp.where(
        lax.axis_index("col") > 0, predicted[:, :, :1] - before[:outputs] - before[outputs:], 0.0
    )
    row_prior = jnp.concatenate([above, row_error[:, :-1, :]], axis=1)
    col_prior = jnp.concatenate([before, col_error[:, :, :-1]], axis=2)
    cotangent = pixel_cotangent(value_error, row_error, row_prior, col_error, col_prior)
    grad_in, grad_mid, grad_out, feature_grad = decoder_backward(
        features,
        pre_acts,
        activations,
        cotangent.reshape(outputs, sample_rows * sample_cols),
        low_in,
        low_mid,
        low_out,
    )
    fine_back, coarse_back = spread_features(feature_grad, tables)
    side_cols = jnp.concatenate(
        [fine_back[:, :, sample_cols:], coarse_back[:, :, coarse_cols:]], axis=1
    )
    side_cols = shifted(side_cols, "col", 1)
    fine_tall_grad = jnp.concatenate(
        [fine_back[:, :, :1] + side_cols[:, : sample_rows + 1, :], fine_back[:, :, 1:sample_cols]],
        axis=2,
    )
    coarse_tall_grad = jnp.concatenate(
        [
            coarse_back[:, :, :1] + side_cols[:, sample_rows + 1 :, :],
            coarse_back[:, :, 1:coarse_cols],
        ],
        axis=2,
    )
    bottom_rows = jnp.concatenate(
        [fine_tall_grad[:, sample_rows:, :], coarse_tall_grad[:, coarse_rows:, :]], axis=2
    )
    bottom_rows = shifted(bottom_rows, "row", 1)
    fine_grad = jnp.concatenate(
        [
            fine_tall_grad[:, :1, :] + bottom_rows[:, :, :sample_cols],
            fine_tall_grad[:, 1:sample_rows, :],
        ],
        axis=1,
    )
    coarse_grad = jnp.concatenate(
        [
            coarse_tall_grad[:, :1, :] + bottom_rows[:, :, sample_cols:],
            coarse_tall_grad[:, 1:coarse_rows, :],
        ],
        axis=1,
    )
    grid_local = jnp.sum(fine_grad * fine_grad) + jnp.sum(coarse_grad * coarse_grad)
    devices = lax.axis_size("row") * lax.axis_size("col")
    grid_entries = (fine_grad.size + coarse_grad.size) * devices
    input_step, middle_step, output_step, grid_total = decoder_steps(
        (grad_in, grad_mid, grad_out),
        (in_first, mid_first, out_first),
        (in_second, mid_second, out_second),
        grid_local,
    )
    grid_scale = clip_factor(grid_total, grid_entries)
    fine_step = adam_step(fine_grad, fine_first, fine_second, grid_scale)
    coarse_step = adam_step(coarse_grad, coarse_first, coarse_second, grid_scale)
    return (fine_step, coarse_step, input_step, middle_step, output_step)


def solution(mesh):
    placed = (
        P("row", "col", None),
        P(None, None, "row", "col"),
        P(None, "row", "col"),
        P(None, "row", "col"),
        P(),
        P(),
        P(),
        P(None, "row", "col"),
        P(None, "row", "col"),
        P(None, "row", "col"),
        P(None, "row", "col"),
        P(),
        P(),
        P(),
        P(),
        P(),
        P(),
    )
    return jax.shard_map(
        shards,
        mesh=mesh,
        in_specs=placed,
        out_specs=(P(None, "row", "col"), P(None, "row", "col"), P(), P(), P()),
        check_vma=False,
    )
```
